32 devices in a mesh: tp: 4 (over z), dp: 8 (over y, x, core).
Axes of the slice: x: 2, y: 2, z: 4, core: 2. Of those that a mesh axis runs over, the one named last changes fastest.
Arguments:
- hidden: bfloat16 [2048, 896], P('dp')
- norm_w: bfloat16 [896], replicated
- emb_table: bfloat16 [151936, 896], P('tp')
- teacher: bfloat16 [2048, 151936], P('dp', 'tp')
- loss_mask: int32 [2048], P('dp')
Outputs:
- output 1: float32 [], replicated
- output 2: bfloat16 [2048, 896], P('dp')
- output 3: float32 [151936, 896], P('tp', 'dp')
- output 4: float32 [896], replicated
All inputs are finite; a program needn't handle non-finite values.
Results may differ from the reference program's by a relative error of at most 0.001.
Values sent between devices are 32-bit elements.
A program may use at most 1 GiB of HBM per device.

```python
import jax
import jax.numpy as jnp
from jax import lax

MODEL_DIM = 896
VOCAB_SIZE = 151936
TOK_DEV = 256
DP_SHARDS = 8
TOKENS = TOK_DEV * DP_SHARDS
SOFT_CAP = 30.0
NORM_EPS = 1e-6


def setup_inputs(seed: int = 0) -> dict:
    base_key = jax.random.key(seed)
    key_list = jax.random.split(base_key, 6)
    hidden = jax.random.normal(key_list[0], (TOKENS, MODEL_DIM), jnp.float32)
    norm_w = 0.5 * jax.random.normal(key_list[1], (MODEL_DIM,), jnp.float32)
    mean_dir = jax.random.normal(key_list[2], (MODEL_DIM,), jnp.float32)
    emb_noise = jax.random.normal(key_list[3], (VOCAB_SIZE, MODEL_DIM), jnp.float32)
    emb_table = (18.0 * mean_dir[None, :] + 1.5 * emb_noise) * (MODEL_DIM ** -0.5)
    teacher = 2.0 * jax.random.normal(key_list[4], (TOKENS, VOCAB_SIZE), jnp.float32)
    lengths = jax.random.randint(key_list[5], (DP_SHARDS,), 1, TOK_DEV + 1)
    lengths = jnp.where(jnp.arange(DP_SHARDS) == 0, TOK_DEV, lengths)
    loss_mask = (jnp.arange(TOK_DEV)[None, :] < lengths[:, None]).astype(jnp.int32)
    return {'hidden': hidden.astype(jnp.bfloat16), 'norm_w': norm_w.astype(jnp.bfloat16), 'emb_table': emb_table.astype(jnp.bfloat16), 'teacher': teacher.astype(jnp.bfloat16), 'loss_mask': loss_mask.reshape(TOKENS)}


def rms_norm(hid_f32, scale_f32):
    inv_rms = lax.rsqrt(jnp.mean(hid_f32 * hid_f32, axis=-1, keepdims=True) + NORM_EPS)
    return hid_f32 * inv_rms * (1.0 + scale_f32)


def reference(hidden, norm_w, emb_table, teacher, loss_mask):
    mask_f32 = loss_mask.astype(jnp.float32)
    weights = mask_f32 / jnp.sum(mask_f32)
    scale_f32 = norm_w.astype(jnp.float32)

    def block_step(acc_state, blk_inputs):
        emb_acc, scale_acc = acc_state
        hid_blk, teach_blk, weight_blk = blk_inputs
        normed_f32, norm_pull = jax.vjp(rms_norm, hid_blk.astype(jnp.float32), scale_f32)
        normed = normed_f32.astype(jnp.bfloat16)
        raw_logit = jnp.dot(normed, emb_table.T, preferred_element_type=jnp.float32)
        tanh_val = jnp.tanh(raw_logit / SOFT_CAP)
        capped = SOFT_CAP * tanh_val
        log_stu = jax.nn.log_softmax(capped, axis=-1)
        log_tea = jax.nn.log_softmax(teach_blk.astype(jnp.float32), axis=-1)
        prob_tea = jnp.exp(log_tea)
        kl_tok = jnp.sum(prob_tea * (log_tea - log_stu), axis=-1)
        loss_part = jnp.sum(weight_blk * kl_tok)
        d_raw = ((jnp.exp(log_stu) - prob_tea) * weight_blk[:, None] * (1.0 - tanh_val * tanh_val)).astype(jnp.bfloat16)
        grad_normed = jnp.dot(d_raw, emb_table, preferred_element_type=jnp.float32)
        emb_acc = emb_acc + jnp.dot(d_raw.T, normed, preferred_element_type=jnp.float32)
        grad_hid, grad_scale = norm_pull(grad_normed)
        return (emb_acc, scale_acc + grad_scale), (loss_part, grad_hid.astype(jnp.bfloat16))

    blocks_in = (hidden.reshape(DP_SHARDS, TOK_DEV, MODEL_DIM), teacher.reshape(DP_SHARDS, TOK_DEV, VOCAB_SIZE), weights.reshape(DP_SHARDS, TOK_DEV))
    start_acc = (jnp.zeros((VOCAB_SIZE, MODEL_DIM), jnp.float32), jnp.zeros((MODEL_DIM,), jnp.float32))
    final_acc, per_block = lax.scan(block_step, start_acc, blocks_in)
    d_emb, d_norm_w = final_acc
    loss_parts, grad_hid = per_block
    return jnp.sum(loss_parts), grad_hid.reshape(TOKENS, MODEL_DIM), d_emb, d_norm_w
```

```python
import functools

import jax
import jax.numpy as jnp
from jax import lax
from jax.experimental import pallas as pl
from jax.experimental.pallas import tpu as pltpu
from jax.sharding import PartitionSpec as P

SOFT_CAP = 30.0
NORM_EPS = 1e-6
LOG2E = 1.4426950408889634
CAP2 = SOFT_CAP * LOG2E
CHUNKS = 10
HALF = 1920
ROWS_F = 1024
ROWS_B = 960
ROWS_M = 640


def rms_norm(hid_f32, scale_f32):
    inv_rms = lax.rsqrt(jnp.mean(hid_f32 * hid_f32, axis=-1, keepdims=True) + NORM_EPS)
    return hid_f32 * inv_rms * (1.0 + scale_f32)


def sublane_sum(a):
    return jnp.sum(a, axis=0, keepdims=True)


def stats_kernel(vocab, e_ref, t_ref, g_ref, out_ref):
    i = pl.program_id(0)
    n = pl.num_programs(0)
    rows = e_ref.shape[0]

    @pl.when(i == 0)
    def _():
        out_ref[...] = jnp.zeros_like(out_ref)
        out_ref[1:2, :] = jnp.full((1, out_ref.shape[1]), -jnp.inf, jnp.float32)

    def block(ragged):
        raw = jnp.dot(e_ref[...], g_ref[...], preferred_element_type=jnp.float32)
        u = jnp.tanh(raw * (1.0 / SOFT_CAP))
        ez = jnp.exp2(u * CAP2 - CAP2)
        t = t_ref[...].astype(jnp.float32)
        if ragged:
            valid = lax.broadcasted_iota(jnp.int32, t.shape, 0) < vocab - i * rows
            t = jnp.where(valid, t, -jnp.inf)
        top_old = out_ref[1:2, :]
        top = jnp.maximum(top_old, jnp.max(t, axis=0, keepdims=True))
        et = jnp.exp2((t - top) * LOG2E)
        cross = et * (t - SOFT_CAP * u)
        if ragged:
            ez = jnp.where(valid, ez, 0.0)
            cross = jnp.where(valid, cross, 0.0)
        keep = jnp.exp2((top_old - top) * LOG2E)
        out_ref[0:1, :] += sublane_sum(ez)
        out_ref[1:2, :] = top
        out_ref[2:3, :] = out_ref[2:3, :] * keep + sublane_sum(et)
        out_ref[3:4, :] = out_ref[3:4, :] * keep + sublane_sum(cross)

    if vocab % rows:
        pl.when(i < n - 1)(lambda: block(False))
        pl.when(i == n - 1)(lambda: block(True))
    else:
        block(False)


def local_stats(emb, teach_t, g_t):
    vocab, dim = emb.shape
    tok = teach_t.shape[1]
    return pl.pallas_call(
        functools.partial(stats_kernel, vocab),
        out_shape=jax.ShapeDtypeStruct((8, tok), jnp.float32),
        grid=(pl.cdiv(vocab, ROWS_F),),
        in_specs=[
            pl.BlockSpec((ROWS_F, dim), lambda i: (i, 0)),
            pl.BlockSpec((ROWS_F, tok), lambda i: (i, 0)),
            pl.BlockSpec((dim, tok), lambda i: (0, 0)),
        ],
        out_specs=pl.BlockSpec((8, tok), lambda i: (0, 0)),
        cost_estimate=pl.CostEstimate(
            flops=2 * vocab * dim * tok, bytes_accessed=2 * vocab * (dim + tok), transcendentals=3 * vocab * tok
        ),
        name="stats",
    )(emb, teach_t, g_t)


def grad_kernel(limit, first, nb, side_ref, e_ref, t_ref, g_ref, st_ref, acc_ref, send_ref, own_ref, dg_ref):
    h, j = pl.program_id(0), pl.program_id(1)
    rows = e_ref.shape[0]

    @pl.when((h == 0) & (j == 0))
    def _():
        dg_ref[...] = acc_ref[...]

    emb = e_ref[...]
    raw = jnp.dot(emb, g_ref[...], preferred_element_type=jnp.float32)
    u = jnp.tanh(raw * (1.0 / SOFT_CAP))
    ez = jnp.exp2(u * CAP2 - CAP2)
    et = jnp.exp2((t_ref[...].astype(jnp.float32) - st_ref[1:2, :]) * LOG2E)
    dr = (ez * st_ref[0:1, :] - et * st_ref[2:3, :]) * (1.0 - u * u)
    if limit is not None:
        half = jnp.where(h == 0, 1 - side_ref[0], side_ref[0])
        left = limit - (first + half * nb + j) * rows
        dr = jnp.where(lax.broadcasted_iota(jnp.int32, dr.shape, 0) < left, dr, 0.0)
        emb = jnp.where(lax.broadcasted_iota(jnp.int32, emb.shape, 0) < left, emb, jnp.zeros_like(emb))
    dr = dr.astype(jnp.bfloat16)
    wide = dr.astype(jnp.float32)

    @pl.when(h == 0)
    def _():
        send_ref[...] = wide

    @pl.when(h == 1)
    def _():
        own_ref[...] = wide

    dg_ref[...] += lax.dot_general(dr, emb, (((0,), (0,)), ((), ())), preferred_element_type=jnp.float32)


def chunk_grad(chunk, side, emb, teach_t, g_t, stats, acc):
    vocab, dim = emb.shape
    tok = teach_t.shape[1]
    nb = HALF // ROWS_B
    first = chunk * 2 * nb
    limit = vocab if (chunk + 1) * 2 * HALF > vocab else None

    def rows_map(h, j, side_ref):
        half = jnp.where(h == 0, 1 - side_ref[0], side_ref[0])
        return first + half * nb + j, 0

    whole = lambda h, j, side_ref: (0, 0)
    half_shape = jax.ShapeDtypeStruct((HALF, tok), jnp.float32)
    return pl.pallas_call(
        functools.partial(grad_kernel, limit, first, nb),
        out_shape=(half_shape, half_shape, jax.ShapeDtypeStruct((tok, dim), jnp.float32)),
        grid_spec=pltpu.PrefetchScalarGridSpec(
            num_scalar_prefetch=1,
            grid=(2, nb),
            in_specs=[
                pl.BlockSpec((ROWS_B, dim), rows_map),
                pl.BlockSpec((ROWS_B, tok), rows_map),
                pl.BlockSpec((dim, tok), whole),
                pl.BlockSpec((8, tok), whole),
                pl.BlockSpec((tok, dim), whole),
            ],
            out_specs=(
                pl.BlockSpec((ROWS_B, tok), lambda h, j, s: (jnp.where(h == 0, j, nb - 1), 0)),
                pl.BlockSpec((ROWS_B, tok), lambda h, j, s: (jnp.where(h == 0, 0, j), 0)),
                pl.BlockSpec((tok, dim), whole),
            ),
        ),
        cost_estimate=pl.CostEstimate(
            flops=8 * HALF * dim * tok, bytes_accessed=4 * HALF * (dim + 3 * tok), transcendentals=6 * HALF * tok
        ),
        name="grad",
    )(side, emb, teach_t, g_t, stats, acc)


def table_kernel(own_ref, near_ref, core_ref, far_ref, g_ref, send_ref, keep_ref, pass_ref, held):
    part = keep_ref.shape[0]

    @pl.when(pl.program_id(0) == 0)
    def _():
        held[...] = g_ref[...].astype(jnp.bfloat16)

    dr = jnp.concatenate([r[...].astype(jnp.bfloat16) for r in (own_ref, near_ref, core_ref, far_ref)], axis=1)
    out = lax.dot_general(held[...], dr, (((1,), (1,)), ((), ())), preferred_element_type=jnp.float32)
    send_ref[...] = out[: 2 * part]
    keep_ref[...] = out[2 * part : 3 * part]
    pass_ref[...] = out[3 * part :]


def chunk_table(pieces, g_rows):
    rows, tok = pieces[0].shape
    width, depth = g_rows.shape
    part = width // 4
    shape = lambda k: jax.ShapeDtypeStruct((k * part, rows), jnp.float32)
    out_spec = lambda k: pl.BlockSpec((k * part, ROWS_M), lambda i: (0, i))
    return pl.pallas_call(
        table_kernel,
        out_shape=(shape(2), shape(1), shape(1)),
        grid=(rows // ROWS_M,),
        in_specs=[pl.BlockSpec((ROWS_M, tok), lambda i: (i, 0))] * 4 + [pl.BlockSpec((width, depth), lambda i: (0, 0))],
        out_specs=(out_spec(2), out_spec(1), out_spec(1)),
        scratch_shapes=[pltpu.VMEM((width, depth), jnp.bfloat16)],
        cost_estimate=pl.CostEstimate(
            flops=2 * width * depth * rows, bytes_accessed=4 * rows * (4 * tok + width), transcendentals=0
        ),
        name="table",
    )(*pieces, g_rows)


def solution(mesh):
    dp = mesh.shape['dp']
    bits = {'core': 1, 'x': 2, 'y': 4}

    def swap(a, axis):
        return lax.ppermute(a, 'dp', [(i, i ^ bits[axis]) for i in range(dp)])

    def device_fn(hid_loc, norm_w, emb_loc, teach_loc, mask_loc):
        vocab, dim = emb_loc.shape
        me = lax.axis_index('dp')
        place = {axis: (me // bit) % 2 for axis, bit in bits.items()}
        mask_f32 = mask_loc.astype(jnp.float32)
        tok_count = lax.psum(jnp.sum(mask_f32), 'dp')
        weight = mask_f32 / tok_count
        normed_f32, norm_pull = jax.vjp(rms_norm, hid_loc.astype(jnp.float32), norm_w.astype(jnp.float32))
        normed = lax.optimization_barrier(normed_f32.astype(jnp.bfloat16))
        g_t = normed.T
        teach_t = teach_loc.T

        g_own = normed.astype(jnp.float32)
        near = {axis: swap(g_own, axis) for axis in 'xy'}
        g_core = swap(g_own, 'core')

        def g_rows(a, b):
            g_all = jnp.concatenate([g_own, near[a], g_core, swap(near[a], 'core')], axis=0)
            cols = g_all.T.reshape(2, 2, 2, dim // 8, g_all.shape[0])
            cols = jnp.where(place['core'] == 0, cols[:, :, 0], cols[:, :, 1])
            cols = jnp.where(place['x'] == 0, cols, cols[:, ::-1])
            cols = jnp.where(place['y'] == 0, cols, cols[::-1])
            if b == 'x':
                cols = jnp.swapaxes(cols, 0, 1)
            return cols[::-1].reshape(dim // 2, g_all.shape[0])

        rows_of = {'x': g_rows('x', 'y'), 'y': g_rows('y', 'x')}

        own_stats = local_stats(emb_loc, teach_t, g_t)
        all_stats = lax.all_gather(own_stats[:4], 'tp')
        sum_stu = jnp.sum(all_stats[:, 0], axis=0)
        top = jnp.max(all_stats[:, 1], axis=0)
        scale = jnp.exp(all_stats[:, 1] - top)
        sum_tea = jnp.sum(all_stats[:, 2] * scale, axis=0)
        cross = jnp.sum(all_stats[:, 3] * scale, axis=0)
        kl_tok = cross / sum_tea - (top + jnp.log(sum_tea)) + (SOFT_CAP + jnp.log(sum_stu))
        loss_val = lax.psum(jnp.sum(weight * kl_tok), 'dp')
        stats = jnp.stack([weight / sum_stu, top, weight / sum_tea] + [jnp.zeros_like(top)] * 5)

        grad_part = jnp.zeros(hid_loc.shape, jnp.float32)
        side = {axis: place[axis].astype(jnp.int32)[None] for axis in 'xy'}
        grad_emb = jnp.zeros((dim // 8, vocab), jnp.float32)
        for chunk in range(CHUNKS):
            a, b = ('x', 'y') if chunk % 2 == 0 else ('y', 'x')
            send, own, grad_part = chunk_grad(chunk, side[a], emb_loc, teach_t, g_t, stats, grad_part)
            got = swap(send, a)
            pieces = (own, got, swap(own, 'core'), swap(got, 'core'))
            send_b, keep, give = chunk_table(pieces, rows_of[a])
            got_b = swap(send_b, b)
            mine = keep + got_b[: dim // 8]
            other = swap(give + got_b[dim // 8 :], a)
            low = jnp.where(place[a] == 0, mine, other)
            high = jnp.where(place[a] == 0, other, mine)
            start = chunk * 2 * HALF
            grad_emb = lax.dynamic_update_slice(grad_emb, low, (0, start))
            stop = min(vocab, start + 2 * HALF)
            grad_emb = lax.dynamic_update_slice(grad_emb, high[:, : stop - start - HALF], (0, start + HALF))

        grad_normed = lax.psum(grad_part, 'tp')
        grad_hid, grad_scale = norm_pull(grad_normed)
        grad_w = lax.psum(grad_scale, 'dp')
        return loss_val, grad_hid.astype(jnp.bfloat16), grad_emb.T, grad_w


    return jax.shard_map(device_fn, mesh=mesh, in_specs=(P('dp', None), P(None), P('tp', None), P('dp', 'tp'), P('dp')), out_specs=(P(), P('dp', None), P('tp', 'dp'), P(None)), check_vma=False)
```

```python
import functools

import jax
import jax.numpy as jnp
from jax import lax
from jax.experimental import pallas as pl
from jax.experimental.pallas import tpu as pltpu
from jax.sharding import PartitionSpec as P

SOFT_CAP = 30.0
NORM_EPS = 1e-6
LOG2E = 1.4426950408889634
CAP2 = SOFT_CAP * LOG2E
CHUNKS = 10
EARLY = 4
HALF = 1920
ROWS_F = 1024
ROWS_B = 960
ROWS_M = 640


def rms_norm(hid_f32, scale_f32):
    inv_rms = lax.rsqrt(jnp.mean(hid_f32 * hid_f32, axis=-1, keepdims=True) + NORM_EPS)
    return hid_f32 * inv_rms * (1.0 + scale_f32)


def sublane_sum(a):
    return jnp.sum(a, axis=0, keepdims=True)


def stats_kernel(vocab, e_ref, t_ref, g_ref, out_ref):
    i = pl.program_id(0)
    n = pl.num_programs(0)
    rows = e_ref.shape[0]

    @pl.when(i == 0)
    def _():
        out_ref[...] = jnp.zeros_like(out_ref)
        out_ref[1:2, :] = jnp.full((1, out_ref.shape[1]), -jnp.inf, jnp.float32)

    def block(ragged):
        raw = jnp.dot(e_ref[...], g_ref[...], preferred_element_type=jnp.float32)
        u = jnp.tanh(raw * (1.0 / SOFT_CAP))
        ez = jnp.exp2(u * CAP2 - CAP2)
        t = t_ref[...].astype(jnp.float32)
        if ragged:
            valid = lax.broadcasted_iota(jnp.int32, t.shape, 0) < vocab - i * rows
            t = jnp.where(valid, t, -jnp.inf)
        top_old = out_ref[1:2, :]
        top = jnp.maximum(top_old, jnp.max(t, axis=0, keepdims=True))
        et = jnp.exp2((t - top) * LOG2E)
        cross = et * (t - SOFT_CAP * u)
        if ragged:
            ez = jnp.where(valid, ez, 0.0)
            cross = jnp.where(valid, cross, 0.0)
        keep = jnp.exp2((top_old - top) * LOG2E)
        out_ref[0:1, :] += sublane_sum(ez)
        out_ref[1:2, :] = top
        out_ref[2:3, :] = out_ref[2:3, :] * keep + sublane_sum(et)
        out_ref[3:4, :] = out_ref[3:4, :] * keep + sublane_sum(cross)

    if vocab % rows:
        pl.when(i < n - 1)(lambda: block(False))
        pl.when(i == n - 1)(lambda: block(True))
    else:
        block(False)


def local_stats(emb, teach_t, g_t):
    vocab, dim = emb.shape
    tok = teach_t.shape[1]
    return pl.pallas_call(
        functools.partial(stats_kernel, vocab),
        out_shape=jax.ShapeDtypeStruct((8, tok), jnp.float32),
        grid=(pl.cdiv(vocab, ROWS_F),),
        in_specs=[
            pl.BlockSpec((ROWS_F, dim), lambda i: (i, 0)),
            pl.BlockSpec((ROWS_F, tok), lambda i: (i, 0)),
            pl.BlockSpec((dim, tok), lambda i: (0, 0)),
        ],
        out_specs=pl.BlockSpec((8, tok), lambda i: (0, 0)),
        cost_estimate=pl.CostEstimate(
            flops=2 * vocab * dim * tok, bytes_accessed=2 * vocab * (dim + tok), transcendentals=3 * vocab * tok
        ),
        name="stats",
    )(emb, teach_t, g_t)


def logit_grad(emb, t, g_ref, st_ref):
    raw = jnp.dot(emb, g_ref[...], preferred_element_type=jnp.float32)
    u = jnp.tanh(raw * (1.0 / SOFT_CAP))
    ez = jnp.exp2(u * CAP2 - CAP2)
    et = jnp.exp2((t.astype(jnp.float32) - st_ref[1:2, :]) * LOG2E)
    return (ez * st_ref[0:1, :] - et * st_ref[2:3, :]) * (1.0 - u * u)


def grad_kernel(limit, first, nb, side_ref, e_ref, t_ref, g_ref, st_ref, acc_ref, *out_refs):
    *send_refs, own_ref, dg_ref = out_refs
    h, j = pl.program_id(0), pl.program_id(1)
    rows = e_ref.shape[0]

    @pl.when((h == 0) & (j == 0))
    def _():
        dg_ref[...] = acc_ref[...]

    emb = e_ref[...]
    dr = logit_grad(emb, t_ref[...], g_ref, st_ref)
    if limit is not None:
        half = jnp.where(h == 0, 1 - side_ref[0], side_ref[0])
        left = limit - (first + half * nb + j) * rows
        dr = jnp.where(lax.broadcasted_iota(jnp.int32, dr.shape, 0) < left, dr, 0.0)
        emb = jnp.where(lax.broadcasted_iota(jnp.int32, emb.shape, 0) < left, emb, jnp.zeros_like(emb))
    dr = dr.astype(jnp.bfloat16)
    wide = dr.astype(jnp.float32)

    for send_ref in send_refs:

        @pl.when(h == 0)
        def _():
            send_ref[...] = wide

    @pl.when(h == 1)
    def _():
        own_ref[...] = wide

    dg_ref[...] += lax.dot_general(dr, emb, (((0,), (0,)), ((), ())), preferred_element_type=jnp.float32)


def chunk_grad(chunk, send, side, emb, teach_t, g_t, stats, acc):
    vocab, dim = emb.shape
    tok = teach_t.shape[1]
    nb = HALF // ROWS_B
    first = chunk * 2 * nb
    limit = vocab if (chunk + 1) * 2 * HALF > vocab else None

    def rows_map(h, j, side_ref):
        half = jnp.where(h == 0, 1 - side_ref[0], side_ref[0])
        return first + half * nb + j, 0

    whole = lambda h, j, side_ref: (0, 0)
    half_shape = jax.ShapeDtypeStruct((HALF, tok), jnp.float32)
    return pl.pallas_call(
        functools.partial(grad_kernel, limit, first, nb),
        out_shape=(half_shape,) * (2 if send else 1) + (jax.ShapeDtypeStruct((tok, dim), jnp.float32),),
        grid_spec=pltpu.PrefetchScalarGridSpec(
            num_scalar_prefetch=1,
            grid=(2, nb),
            in_specs=[
                pl.BlockSpec((ROWS_B, dim), rows_map),
                pl.BlockSpec((ROWS_B, tok), rows_map),
                pl.BlockSpec((dim, tok), whole),
                pl.BlockSpec((8, tok), whole),
                pl.BlockSpec((tok, dim), whole),
            ],
            out_specs=([pl.BlockSpec((ROWS_B, tok), lambda h, j, s: (jnp.where(h == 0, j, nb - 1), 0))] if send else [])
            + [
                pl.BlockSpec((ROWS_B, tok), lambda h, j, s: (jnp.where(h == 0, 0, j), 0)),
                pl.BlockSpec((tok, dim), whole),
            ],
        ),
        cost_estimate=pl.CostEstimate(
            flops=8 * HALF * dim * tok, bytes_accessed=4 * HALF * (dim + 3 * tok), transcendentals=6 * HALF * tok
        ),
        name="grad",
    )(side, emb, teach_t, g_t, stats, acc)


def near_kernel(side_ref, e_ref, t_ref, g_ref, st_ref, out_ref):
    dr = logit_grad(e_ref[...], t_ref[...], g_ref, st_ref)
    out_ref[...] = dr.astype(jnp.bfloat16).astype(jnp.float32)


def near_grad(chunk, side, emb, teach_near, g_t, stats):
    rows, tok = teach_near.shape
    dim = emb.shape[1]
    nb = rows // ROWS_B
    whole = lambda j, side_ref: (0, 0)
    return pl.pallas_call(
        near_kernel,
        out_shape=jax.ShapeDtypeStruct((rows, tok), jnp.float32),
        grid_spec=pltpu.PrefetchScalarGridSpec(
            num_scalar_prefetch=1,
            grid=(nb,),
            in_specs=[
                pl.BlockSpec((ROWS_B, dim), lambda j, side_ref: ((2 * chunk + side_ref[0]) * nb + j, 0)),
                pl.BlockSpec((ROWS_B, tok), lambda j, side_ref: (j, 0)),
                pl.BlockSpec((dim, tok), whole),
                pl.BlockSpec((8, tok), whole),
            ],
            out_specs=pl.BlockSpec((ROWS_B, tok), lambda j, side_ref: (j, 0)),
        ),
        cost_estimate=pl.CostEstimate(
            flops=2 * rows * dim * tok, bytes_accessed=2 * rows * (dim + 4 * tok), transcendentals=3 * rows * tok
        ),
        name="near",
    )(side, emb, teach_near, g_t, stats)


def widen_kernel(side_ref, t_ref, out_ref):
    out_ref[...] = t_ref[...].astype(jnp.float32)


def widen_half(chunk, side, teach_t):
    tok = teach_t.shape[1]
    nb = HALF // ROWS_B
    return pl.pallas_call(
        widen_kernel,
        out_shape=jax.ShapeDtypeStruct((HALF, tok), jnp.float32),
        grid_spec=pltpu.PrefetchScalarGridSpec(
            num_scalar_prefetch=1,
            grid=(nb,),
            in_specs=[pl.BlockSpec((ROWS_B, tok), lambda j, side_ref: ((2 * chunk + 1 - side_ref[0]) * nb + j, 0))],
            out_specs=pl.BlockSpec((ROWS_B, tok), lambda j, side_ref: (j, 0)),
        ),
        cost_estimate=pl.CostEstimate(flops=HALF * tok, bytes_accessed=6 * HALF * tok, transcendentals=0),
        name="widen",
    )(side, teach_t)


def place_kernel(side_ref, mine_ref, other_ref, *refs):
    out_ref = refs[-1]

    @pl.when(pl.program_id(0) == 0)
    def _():
        out_ref[...] = mine_ref[...]

    @pl.when(pl.program_id(0) == 1)
    def _():
        out_ref[...] = other_ref[...]


def place(chunk, side, mine, other, vocab, out):
    cols, rows = mine.shape
    whole = lambda h, side_ref: (0, 0)
    given = [] if out is None else [out]
    return pl.pallas_call(
        place_kernel,
        out_shape=jax.ShapeDtypeStruct((cols, vocab), jnp.float32),
        grid_spec=pltpu.PrefetchScalarGridSpec(
            num_scalar_prefetch=1,
            grid=(2,),
            in_specs=[pl.BlockSpec((cols, rows), whole)] * 2 + [pl.BlockSpec(memory_space=pl.ANY)] * len(given),
            out_specs=pl.BlockSpec(
                (cols, rows), lambda h, side_ref: (0, 2 * chunk + jnp.where(h == 0, side_ref[0], 1 - side_ref[0]))
            ),
        ),
        input_output_aliases={3: 0} if given else {},
        cost_estimate=pl.CostEstimate(flops=cols * rows, bytes_accessed=16 * cols * rows, transcendentals=0),
        name="place",
    )(side, mine, other, *given)


def table_kernel(own_ref, near_ref, core_ref, far_ref, g_ref, send_ref, keep_ref, pass_ref, held):
    part = keep_ref.shape[0]

    @pl.when(pl.program_id(0) == 0)
    def _():
        held[...] = g_ref[...].astype(jnp.bfloat16)

    dr = jnp.concatenate([r[...].astype(jnp.bfloat16) for r in (own_ref, near_ref, core_ref, far_ref)], axis=1)
    out = lax.dot_general(held[...], dr, (((1,), (1,)), ((), ())), preferred_element_type=jnp.float32)
    send_ref[...] = out[: 2 * part]
    keep_ref[...] = out[2 * part : 3 * part]
    pass_ref[...] = out[3 * part :]


def chunk_table(pieces, g_rows):
    rows, tok = pieces[0].shape
    width, depth = g_rows.shape
    part = width // 4
    shape = lambda k: jax.ShapeDtypeStruct((k * part, rows), jnp.float32)
    out_spec = lambda k: pl.BlockSpec((k * part, ROWS_M), lambda i: (0, i))
    return pl.pallas_call(
        table_kernel,
        out_shape=(shape(2), shape(1), shape(1)),
        grid=(rows // ROWS_M,),
        in_specs=[pl.BlockSpec((ROWS_M, tok), lambda i: (i, 0))] * 4 + [pl.BlockSpec((width, depth), lambda i: (0, 0))],
        out_specs=(out_spec(2), out_spec(1), out_spec(1)),
        scratch_shapes=[pltpu.VMEM((width, depth), jnp.bfloat16)],
        cost_estimate=pl.CostEstimate(
            flops=2 * width * depth * rows, bytes_accessed=4 * rows * (4 * tok + width), transcendentals=0
        ),
        name="table",
    )(*pieces, g_rows)


def solution(mesh):
    dp, tp = mesh.shape['dp'], mesh.shape['tp']
    bits = {'core': 1, 'x': 2, 'y': 4}

    def trade(a, axis, mask):
        size = mesh.shape[axis]
        return lax.ppermute(a, axis, [(i, i ^ mask) for i in range(size)])

    def swap(a, link):
        return trade(a, 'dp', bits[link])

    def tree(parts, join):
        while len(parts) > 1:
            parts = [join(parts[i], parts[i + 1]) for i in range(0, len(parts), 2)]
        return parts[0]

    def join_stats(one, two):
        top = jnp.maximum(one[1], two[1])
        first, second = jnp.exp(one[1] - top), jnp.exp(two[1] - top)
        return (
            one[0] + two[0],
            top,
            one[2] * first + two[2] * second,
            one[3] * first + two[3] * second,
        )

    late = list(range(EARLY, CHUNKS))
    early = list(range(EARLY))
    axes = [('x', 'y') if chunk % 2 == 0 else ('y', 'x') for chunk in range(CHUNKS)]

    def device_fn(hid_loc, norm_w, emb_loc, teach_loc, mask_loc):
        vocab, dim = emb_loc.shape
        me = lax.axis_index('dp')
        place_of = {axis: (me // bit) % 2 for axis, bit in bits.items()}
        side = {axis: place_of[axis].astype(jnp.int32)[None] for axis in 'xy'}
        mask_f32 = mask_loc.astype(jnp.float32)
        own_count = jnp.full((8, 128), jnp.sum(mask_f32))
        tok_count = tree([own_count] + [trade(own_count, 'dp', k) for k in range(1, dp)], jnp.add)[0, 0]
        weight = mask_f32 / tok_count
        normed_f32, norm_pull = jax.vjp(rms_norm, hid_loc.astype(jnp.float32), norm_w.astype(jnp.float32))
        normed = lax.optimization_barrier(normed_f32.astype(jnp.bfloat16))
        g_t = normed.T
        teach_t = teach_loc.T

        g_own = normed.astype(jnp.float32)
        near = {axis: swap(g_own, axis) for axis in 'xy'}
        g_core = swap(g_own, 'core')
        teach_near = []
        for chunk in early:
            a = axes[chunk][0]
            wide = widen_half(chunk, side[a], teach_t)
            teach_near.append(swap(wide, a))

        def g_rows(a, b):
            g_all = jnp.concatenate([g_own, near[a], g_core, swap(near[a], 'core')], axis=0)
            cols = g_all.T.reshape(2, 2, 2, dim // 8, g_all.shape[0])
            cols = jnp.where(place_of['core'] == 0, cols[:, :, 0], cols[:, :, 1])
            cols = jnp.where(place_of['x'] == 0, cols, cols[:, ::-1])
            cols = jnp.where(place_of['y'] == 0, cols, cols[::-1])
            if b == 'x':
                cols = jnp.swapaxes(cols, 0, 1)
            return cols[::-1].reshape(dim // 2, g_all.shape[0])

        rows_of = {'x': g_rows('x', 'y'), 'y': g_rows('y', 'x')}

        own_stats = local_stats(emb_loc, teach_t, g_t)
        all_stats = [own_stats] + [trade(own_stats, 'tp', k) for k in range(1, tp)]
        sum_stu, top, sum_tea, cross = tree([tuple(st[i] for i in range(4)) for st in all_stats], join_stats)
        kl_tok = cross / sum_tea - (top + jnp.log(sum_tea)) + (SOFT_CAP + jnp.log(sum_stu))
        loss_part = jnp.sum(weight * kl_tok)
        stats = jnp.stack([weight / sum_stu, top, weight / sum_tea] + [jnp.zeros_like(top)] * 5)
        stats_near = {axis: swap(stats, axis) for axis in 'xy'}
        g_near_t = {axis: lax.optimization_barrier(near[axis]).T.astype(jnp.bfloat16) for axis in 'xy'}

        grad_part = jnp.zeros(hid_loc.shape, jnp.float32)
        pieces = {}
        for chunk in late + early:
            a = axes[chunk][0]
            *send, own, grad_part = chunk_grad(chunk, chunk in late, side[a], emb_loc, teach_t, g_t, stats, grad_part)
            if chunk in late:
                got = swap(send[0], a)
            else:
                got = near_grad(chunk, side[a], emb_loc, teach_near[chunk], g_near_t[a], stats_near[a])
            pieces[chunk] = (own, got, swap(own, 'core'), swap(got, 'core'))

        grad_emb = None
        for chunk in range(CHUNKS):
            a, b = axes[chunk]
            send_b, keep, give = chunk_table(pieces[chunk], rows_of[a])
            got_b = swap(send_b, b)
            mine = keep + got_b[: dim // 8]
            give = give + got_b[dim // 8 :]
            other = swap(give, a)
            grad_emb = place(chunk, side[a], mine, other, vocab, grad_emb)

        grad_normed = grad_part
        for k in range(tp.bit_length() - 1):
            grad_normed = grad_normed + trade(grad_normed, 'tp', 1 << k)
        grad_hid, grad_scale = norm_pull(grad_normed)
        loss_val, grad_w = lax.psum((loss_part, grad_scale), 'dp')
        return loss_val, grad_hid.astype(jnp.bfloat16), grad_emb.T, grad_w

    return jax.shard_map(device_fn, mesh=mesh, in_specs=(P('dp', None), P(None), P('tp', None), P('dp', 'tp'), P('dp')), out_specs=(P(), P('dp', None), P('tp', 'dp'), P(None)), check_vma=False)
```
